32 devices in a mesh: dp: 8 (over z, x), mp: 4 (over y, core).
Axes of the slice: x: 2, y: 2, z: 4, core: 2. Of those that a mesh axis runs over, the one named last changes fastest.
Arguments:
- hidden_activation: bfloat16 [2, 8, 2, 256, 14336], P(None, 'dp', None, None, 'mp'), may hold values from -6 to 6
- target_head_rows: bfloat16 [2, 8, 2, 256, 4096], P(None, 'dp', None, None, 'mp'), may hold values from -6 to 6
- reference_log_probability: float32 [2, 8, 2, 256], P(None, 'dp'), may hold values from -8 to -0.05
- response_token_mask: int32 [2, 8, 2, 256], P(None, 'dp'), may hold values 0 or 1
- sequence_tile_lengths: int32 [2, 8, 2], P(None, 'dp'), may hold values from 1 to 2
- pair_destination: int32 [2, 8], replicated, may hold values from 0 to 7, each once within a row
- adapter_down_first: bfloat16 [14336, 256], P('mp'), may hold values from -0.046875 to 0.046875
- adapter_down_second: bfloat16 [4096, 256], P('mp'), may hold values from -0.09375 to 0.09375
Outputs:
- pair_margin: float32 [2, 8], P(None, 'dp')
- mean_loss: float32 [], replicated
- grad_a: float32 [14336, 256], P(('mp', 'dp'))
- grad_b: float32 [4096, 256], P(('mp', 'dp'))
The draws below stay inside these ranges and needn't reach their ends.
Inputs may be any that keep to these rules, and one draw needn't show every extreme that they name: Each row of pair_destination is a permutation of 0 to 7.
All inputs are finite; a program needn't handle non-finite values. No bound on the sum of `response_token_mask` on one device may be relied on, other than what follows from the above.
Results may differ from the reference program's by a relative error of at most 0.0029.
Values sent between devices are 32-bit elements; how exact they have to be, the bound alone decides.
A program may use at most 128 MiB of HBM per device.

```python
import math
import jax
import jax.numpy as jnp
from jax import lax

MODEL_WIDTH = 4096
HIDDEN_UNITS = 14336
ADAPTER_RANK = 256
TILE = 128
TILES = 2
MICRO = 2
SEQ = 256
PAIRS = 8


def with_ends(result, key, low, high):
    place = [jax.random.randint(jax.random.fold_in(key, axis), (), 0, length) for axis, length in enumerate(result.shape)]
    widest = result.shape.index(max(result.shape))
    beside = place[:widest] + [(place[widest] + 1) % result.shape[widest]] + place[widest + 1:]
    return result.at[tuple(place)].set(low).at[tuple(beside)].set(high)


def shard_levels(own_key, dims, split, low, high):
    def one(axis_at, parts):
        draws = jax.random.uniform(jax.random.fold_in(jax.random.fold_in(own_key, 6), axis_at), (parts,), jnp.float32, low / len(split), high / len(split))
        return jnp.repeat(jnp.exp(draws), dims[axis_at] // parts).reshape((-1,) + (1,) * (len(dims) - axis_at - 1))

    loudness = one(*split[0])
    for cut in split[1:]:
        loudness = loudness * one(*cut)
    return loudness


def centred(rng, extent, spread, limit, split=(), dtype=jnp.bfloat16):
    values = spread * jax.random.normal(rng, extent, jnp.float32)
    if split:
        values = values * shard_levels(rng, extent, split, -0.22, 0.18)
    return jnp.clip(values, -limit, limit).astype(dtype)


def setup_inputs(seed: int = 0) -> dict:
    key_list = jax.random.split(jax.random.key(seed), 9)
    hidden_activation = centred(key_list[0], (MICRO, PAIRS, 2, SEQ, HIDDEN_UNITS), 1.0, 6.0, ((1, 8), (4, 4)))
    target_head_rows = centred(key_list[1], (MICRO, PAIRS, 2, SEQ, MODEL_WIDTH), 1.0, 6.0, ((1, 8), (4, 4)))
    reference_log_probability = jnp.clip(-8.0 + 7.95 * jax.random.uniform(key_list[2], (MICRO, PAIRS, 2, SEQ), jnp.float32) ** shard_levels(key_list[2], (MICRO, PAIRS, 2, SEQ), ((1, 8),), -0.2, 0.2), -8.0, -0.05)
    response_token_mask = with_ends((jax.random.randint(key_list[3], (MICRO, PAIRS, 2, SEQ), 0, 4) < 3).astype(jnp.int32), jax.random.fold_in(key_list[3], 1), 0, 1)
    sequence_tile_lengths = with_ends(jax.random.randint(key_list[4], (MICRO, PAIRS, 2), 1, TILES + 1), jax.random.fold_in(key_list[4], 1), 1, TILES).astype(jnp.int32)
    pair_destination = jax.vmap(lambda own: jax.random.permutation(own, PAIRS))(jax.random.split(key_list[5], MICRO)).reshape((MICRO, PAIRS)).astype(jnp.int32)
    adapter_down_first = centred(key_list[6], (HIDDEN_UNITS, ADAPTER_RANK), HIDDEN_UNITS ** -0.5, 0.046875, ((0, 4),))
    adapter_down_second = centred(key_list[7], (MODEL_WIDTH, ADAPTER_RANK), MODEL_WIDTH ** -0.5, 0.09375, ((0, 4),))
    return {"hidden_activation": hidden_activation, "target_head_rows": target_head_rows, "reference_log_probability": reference_log_probability, "response_token_mask": response_token_mask, "sequence_tile_lengths": sequence_tile_lengths, "pair_destination": pair_destination, "adapter_down_first": adapter_down_first, "adapter_down_second": adapter_down_second}


BETA = 0.1

def pair_loss_terms(hidden_pair, rows_pair, ref_pair, mask_pair, length_pair, weight_a, weight_b):
    hidden_flattened = hidden_pair.reshape(-1, hidden_pair.shape[-1])
    rows_flattened = rows_pair.reshape(-1, rows_pair.shape[-1])
    latent = jnp.dot(hidden_flattened, weight_a, preferred_element_type=jnp.float32)
    readout = jnp.dot(rows_flattened, weight_b, preferred_element_type=jnp.float32)
    rank_square_root = math.sqrt(weight_a.shape[1])
    shift = (lax.optimization_barrier(jnp.sum(latent * readout, axis=-1)) / rank_square_root).reshape(ref_pair.shape)
    chance = jnp.exp(ref_pair)
    denom = 1.0 - chance + chance * jnp.exp(shift)
    gain = shift - jnp.log(denom)
    positions = (jnp.arange(ref_pair.shape[-1]) // TILE).astype(jnp.int32)
    live_mask = ((mask_pair == 1) & (positions[None, :] < length_pair[:, None])).astype(jnp.float32)
    seq_sums = lax.optimization_barrier(jnp.sum(live_mask * gain, axis=-1))
    reward_margin = BETA * (seq_sums[0] - seq_sums[1])
    slope = -jax.nn.sigmoid(-reward_margin)
    signs = jnp.array([1.0, -1.0], jnp.float32)
    factor = live_mask * (slope * BETA) * signs[:, None] * (1.0 - chance) / denom / rank_square_root
    factor = factor.reshape(-1, 1)
    d_latent = (factor * readout).astype(jnp.bfloat16)
    d_readout = (factor * latent).astype(jnp.bfloat16)
    contract = (((0,), (0,)), ((), ()))
    first_portion = lax.dot_general(hidden_flattened, d_latent, contract, preferred_element_type=jnp.float32)
    second_portion = lax.dot_general(rows_flattened, d_readout, contract, preferred_element_type=jnp.float32)
    return (reward_margin, first_portion, second_portion)

def reference(hidden_activation, target_head_rows, reference_log_probability, response_token_mask, sequence_tile_lengths, pair_destination, adapter_down_first, adapter_down_second):
    total_pairs = MICRO * PAIRS
    items = (hidden_activation.reshape(total_pairs, 2, SEQ, HIDDEN_UNITS), target_head_rows.reshape(total_pairs, 2, SEQ, MODEL_WIDTH), reference_log_probability.reshape(total_pairs, 2, SEQ), response_token_mask.reshape(total_pairs, 2, SEQ), sequence_tile_lengths.reshape(total_pairs, 2))

    def advance(carry, pair_entry):
        reward_margin, first_portion, second_portion = pair_loss_terms(pair_entry[0], pair_entry[1], pair_entry[2], pair_entry[3], pair_entry[4], adapter_down_first, adapter_down_second)
        return ((carry[0] + first_portion, carry[1] + second_portion), reward_margin)
    start = (jnp.zeros((HIDDEN_UNITS, ADAPTER_RANK), jnp.float32), jnp.zeros((MODEL_WIDTH, ADAPTER_RANK), jnp.float32))
    (raw_a, raw_b), margins = lax.scan(advance, start, items)
    margins = margins.reshape(MICRO, PAIRS)
    row_index = jnp.arange(MICRO).astype(jnp.int32)[:, None]
    pair_margin = jnp.zeros((MICRO, PAIRS), jnp.float32).at[row_index, pair_destination].set(margins)
    mean_loss = jnp.mean(jax.nn.softplus(-margins))
    squared_values = jnp.sum(raw_a * raw_a) + jnp.sum(raw_b * raw_b)
    adapter_scale = 1.0 / jnp.sqrt(squared_values / (HIDDEN_UNITS * ADAPTER_RANK + MODEL_WIDTH * ADAPTER_RANK) + 1e-06)
    return (pair_margin, mean_loss, raw_a * adapter_scale, raw_b * adapter_scale)
```

```python
import math

import jax
import jax.numpy as jnp
from jax import lax
from jax.sharding import PartitionSpec as P

TILE = 128


BETA = 0.1


def per_device(
    hidden_activation,
    target_head_rows,
    reference_log_probability,
    response_token_mask,
    sequence_tile_lengths,
    pair_destination,
    adapter_down_first,
    adapter_down_second,
):
    micro_count, pairs_dev, _, seq_len, ff_dev = hidden_activation.shape
    d_dev = target_head_rows.shape[-1]
    rank = adapter_down_first.shape[1]
    root = math.sqrt(rank)
    dp_size = lax.axis_size("dp")
    positions = jnp.arange(seq_len) // TILE
    signs = jnp.array([1.0, -1.0], jnp.float32)
    contract = (((0,), (0,)), ((), ()))
    hidden = hidden_activation.reshape(-1, ff_dev)
    rows = target_head_rows.reshape(-1, d_dev)
    latent = jnp.dot(hidden, adapter_down_first, preferred_element_type=jnp.float32)
    readout = jnp.dot(rows, adapter_down_second, preferred_element_type=jnp.float32)
    latent, readout = lax.psum((latent, readout), "mp")
    shift = (jnp.sum(latent * readout, axis=-1) / root).reshape(reference_log_probability.shape)
    chance = jnp.exp(reference_log_probability)
    denom = 1.0 - chance + chance * jnp.exp(shift)
    gain = shift - jnp.log(denom)
    live = (
        (response_token_mask == 1) & (positions < sequence_tile_lengths[..., None])
    ).astype(jnp.float32)
    seq_sums = jnp.sum(live * gain, axis=-1)
    margins = BETA * (seq_sums[..., 0] - seq_sums[..., 1])
    slope = -jax.nn.sigmoid(-margins)
    factor = (
        live
        * (slope * BETA)[..., None, None]
        * signs[:, None]
        * (1.0 - chance)
        / denom
        / root
    ).reshape(-1, 1)
    d_latent = (factor * readout).astype(jnp.bfloat16)
    d_readout = (factor * latent).astype(jnp.bfloat16)
    raw_a = lax.dot_general(hidden, d_latent, contract, preferred_element_type=jnp.float32)
    raw_b = lax.dot_general(rows, d_readout, contract, preferred_element_type=jnp.float32)
    shard_a = lax.psum_scatter(raw_a, "dp", scatter_dimension=0, tiled=True)
    shard_b = lax.psum_scatter(raw_b, "dp", scatter_dimension=0, tiled=True)
    all_margins = lax.all_gather(margins, "dp", axis=1, tiled=True)
    targets = lax.axis_index("dp") * pairs_dev + jnp.arange(pairs_dev)
    hits = pair_destination[:, :, None] == targets[None, None, :]
    pair_margin = jnp.sum(jnp.where(hits, all_margins[:, :, None], 0.0), axis=1)
    mean_loss = jnp.mean(jax.nn.softplus(-all_margins))
    squares = lax.psum(jnp.sum(shard_a * shard_a) + jnp.sum(shard_b * shard_b), ("dp", "mp"))
    count = (ff_dev + d_dev) * rank * lax.axis_size("mp")
    scale = 1.0 / jnp.sqrt(squares / count + 1e-06)
    return (pair_margin, mean_loss, shard_a * scale, shard_b * scale)


def solution(mesh):
    in_specs = (
        P(None, "dp", None, None, "mp"),
        P(None, "dp", None, None, "mp"),
        P(None, "dp", None, None),
        P(None, "dp", None, None),
        P(None, "dp", None),
        P(),
        P("mp", None),
        P("mp", None),
    )
    out_specs = (P(None, "dp"), P(), P(("mp", "dp"), None), P(("mp", "dp"), None))
    return jax.shard_map(
        per_device, mesh=mesh, in_specs=in_specs, out_specs=out_specs, check_vma=False
    )
```

```python
import functools
import math

import jax
import jax.numpy as jnp
from jax import lax
from jax.experimental import pallas as pl
from jax.experimental.pallas import tpu as pltpu
from jax.sharding import PartitionSpec as P

TILE = 128
BETA = 0.1
CORES = 2
SIDES = 2
F32 = jnp.float32
MESH = pl.DeviceIdType.MESH
TRANSPOSED = (((0,), (0,)), ((), ()))


def remote(src, dst, send, recv, target):
    return pltpu.make_async_remote_copy(
        src_ref=src, dst_ref=dst, send_sem=send, recv_sem=recv, device_id=target, device_id_type=MESH
    )


def block_of(size):
    return next(width for width in (512, 256, 128, size) if size % width == 0)


def kernel(
    nd, nm, seq,
    hid_ref, rows_ref, ref_ref, live_ref, wa_ref, wb_ref,
    out_a, out_b, out_stats,
    hid, rows, wa, wb, parts, d2d_in, pair_sum, y_in, full, d_lat, d_read, raw_a, raw_b,
    xin_a, xin_b, zin_a, zin_b, margin_row, mine, mine_dp, stats_mp, stats_dp,
    load_w, load_h, load_r, d2d_s, d2d_r, y_s, y_r, g_s, g_r, x_s, x_r, z_s, z_r, m_s, m_r, p_s, p_r,
):
    tokens, rank = hid.shape[0], wa.shape[1]
    chunks = tokens // seq
    ny, nz = nm // CORES, nd // SIDES
    dp, mp = lax.axis_index("dp"), lax.axis_index("mp")
    core, y = mp % CORES, mp // CORES
    side, z = dp % SIDES, dp // SIDES
    ra, rb = out_a.shape[0], out_b.shape[0]
    root = math.sqrt(rank)

    def span(c):
        return pl.ds(c * seq, seq)

    loads = [
        pltpu.make_async_copy(wa_ref, wa, load_w.at[0]),
        pltpu.make_async_copy(wb_ref, wb, load_w.at[1]),
    ]
    load_hid = [pltpu.make_async_copy(hid_ref.at[span(c)], hid.at[span(c)], load_h.at[c]) for c in range(chunks)]
    load_rows = [pltpu.make_async_copy(rows_ref.at[span(c)], rows.at[span(c)], load_r.at[c]) for c in range(chunks)]
    loads[0].start()
    load_hid[0].start()
    loads[1].start()
    load_rows[0].start()
    for c in range(1, chunks):
        load_hid[c].start()
        load_rows[c].start()

    barrier = pltpu.get_barrier_semaphore()

    @pl.loop(1, nm)
    def _(k):
        pl.semaphore_signal(barrier, inc=1, device_id=(dp, (mp + k) % nm), device_id_type=MESH)

    @pl.loop(1, nd)
    def _(k):
        pl.semaphore_signal(barrier, inc=1, device_id=((dp + k) % nd, mp), device_id_type=MESH)

    pl.semaphore_wait(barrier, nm + nd - 2)

    partner = (dp, y * CORES + (1 - core))

    def d2d_copy(c):
        return remote(parts.at[1 - core, span(c)], d2d_in.at[span(c)], d2d_s.at[c], d2d_r.at[c], partner)

    def y_copy(k, c):
        target = (dp, ((y + k) % ny) * CORES + core)
        return remote(pair_sum.at[span(c)], y_in.at[ny - 1 - k, span(c)], y_s.at[k - 1, c], y_r.at[ny - 1 - k, c], target)

    def g_copy(c):
        return remote(full.at[core, span(c)], full.at[core, span(c)], g_s.at[c], g_r.at[c], partner)

    def g_arrival(c):
        here = full.at[1 - core, span(c)]
        return remote(here, here, g_s.at[c], g_r.at[c], partner)

    def forward(c):
        d2d_copy(c).wait_recv()
        pair_sum[span(c), :] = parts[core, span(c), :] + d2d_in[span(c), :]
        for k in range(1, ny):
            y_copy(k, c).start()

    for c in range(chunks):
        if c == 0:
            loads[0].wait()
        load_hid[c].wait()
        parts[0, span(c), :] = jnp.dot(hid[span(c), :], wa[...], preferred_element_type=F32)
        if c == 0:
            loads[1].wait()
        load_rows[c].wait()
        parts[1, span(c), :] = jnp.dot(rows[span(c), :], wb[...], preferred_element_type=F32)
        d2d_copy(c).start()
        if c:
            forward(c - 1)
    forward(chunks - 1)

    margin_row[...] = jnp.zeros_like(margin_row)
    lane = lax.broadcasted_iota(jnp.int32, margin_row.shape, 1)
    sign = jnp.where(lax.broadcasted_iota(jnp.int32, (2 * seq, 1), 0) < seq, 1.0, -1.0).astype(F32)

    def gradient(both, source, slopes, total, first):
        width = block_of(total.shape[0])

        @pl.loop(0, total.shape[0] // width)
        def _(j):
            at = pl.ds(pl.multiple_of(j * width, width), width)
            term = lax.dot_general(source[both, at], slopes[both, :], TRANSPOSED, preferred_element_type=F32)
            total[at, :] = term if first else total[at, :] + term

    for p in range(chunks // 2):
        for c in (2 * p, 2 * p + 1):
            value = pair_sum[span(c), :]
            for k in range(ny - 1, 0, -1):
                y_copy(k, c).wait_recv()
                value = value + y_in[ny - 1 - k, span(c), :]
            full[core, span(c), :] = value
            g_copy(c).start()
        for c in (2 * p, 2 * p + 1):
            g_arrival(c).wait_recv()
        both = pl.ds(2 * p * seq, 2 * seq)
        latent, readout = full[0, both, :], full[1, both, :]
        shift = jnp.sum(latent * readout, axis=1, keepdims=True) / root
        chance = jnp.exp(ref_ref[both, :])
        denom = 1.0 - chance + chance * jnp.exp(shift)
        gain = shift - jnp.log(denom)
        live = live_ref[both, :]
        margin = BETA * jnp.sum(live * gain * sign, axis=0, keepdims=True)
        slope = -jax.nn.sigmoid(-margin)
        factor = live * (slope * BETA) * sign * (1.0 - chance) / denom / root
        d_lat[both, :] = (factor * readout).astype(jnp.bfloat16)
        d_read[both, :] = (factor * latent).astype(jnp.bfloat16)
        margin_row[...] = jnp.where(lane == p + 1, margin, margin_row[...])
        gradient(both, hid, d_lat, raw_a, p == 0)
        gradient(both, rows, d_read, raw_b, p == 0)

    def at_a(d):
        return pl.ds(pl.multiple_of(d * ra, 8), ra)

    def at_b(d):
        return pl.ds(pl.multiple_of(d * rb, 8), rb)

    def x_copies(k):
        to = (z + 1 + k) % nz
        d = to * SIDES + (1 - side)
        target = (z * SIDES + (1 - side), mp)
        return (
            remote(raw_a.at[at_a(d)], xin_a.at[k], x_s.at[k, 0], x_r.at[k, 0], target),
            remote(raw_b.at[at_b(d)], xin_b.at[k], x_s.at[k, 1], x_r.at[k, 1], target),
        )

    def z_copies(k):
        to = (z + 1 + k) % nz
        target = (to * SIDES + side, mp)
        return (
            remote(xin_a.at[k], zin_a.at[k], z_s.at[k, 0], z_r.at[k, 0], target),
            remote(xin_b.at[k], zin_b.at[k], z_s.at[k, 1], z_r.at[k, 1], target),
        )

    @pl.loop(0, nz)
    def _(k):
        for copy in x_copies(k):
            copy.start()

    @pl.loop(0, nz - 1)
    def _(k):
        d = ((z + 1 + k) % nz) * SIDES + side
        over_a, over_b = x_copies(k)
        on_a, on_b = z_copies(k)
        over_a.wait_recv()
        xin_a[k, :, :] = xin_a[k, :, :] + raw_a[at_a(d), :]
        on_a.start()
        over_b.wait_recv()
        xin_b[k, :, :] = xin_b[k, :, :] + raw_b[at_b(d), :]
        on_b.start()

    over_a, over_b = x_copies(nz - 1)
    over_a.wait_recv()
    out_a[...] = xin_a[nz - 1, :, :] + raw_a[at_a(dp), :]
    over_b.wait_recv()
    out_b[...] = xin_b[nz - 1, :, :] + raw_b[at_b(dp), :]

    @pl.loop(0, nz - 1)
    def _(k):
        on_a, on_b = z_copies(k)
        on_a.wait_recv()
        out_a[...] += zin_a[k, :, :]
        on_b.wait_recv()
        out_b[...] += zin_b[k, :, :]

    def total_of(value):
        return jnp.sum(jnp.sum(value * value, axis=0, keepdims=True), axis=1, keepdims=True)

    mine[0, :, :] = jnp.where(lane == 0, total_of(out_a[...]) + total_of(out_b[...]), margin_row[...])

    def m_copy(k):
        return remote(mine.at[0], stats_mp.at[mp], m_s.at[k - 1], m_r.at[k - 1], (dp, (mp + k) % nm))

    def p_copy(k):
        return remote(mine_dp.at[0], stats_dp.at[dp], p_s.at[k - 1], p_r.at[k - 1], ((dp + k) % nd, mp))

    @pl.loop(1, nm)
    def _(k):
        m_copy(k).start()

    stats_mp[mp, :, :] = mine[0, :, :]

    @pl.loop(1, nm)
    def _(k):
        m_copy(k).wait_recv()

    squares = stats_mp[0, :, :]
    for k in range(1, nm):
        squares = squares + stats_mp[k, :, :]
    mine_dp[0, :, :] = jnp.where(lane == 0, squares, stats_mp[0, :, :])

    @pl.loop(1, nd)
    def _(k):
        p_copy(k).start()

    stats_dp[dp, :, :] = mine_dp[0, :, :]

    @pl.loop(1, nd)
    def _(k):
        p_copy(k).wait_recv()

    out_stats[...] = stats_dp[...]

    for c in range(chunks):
        d2d_copy(c).wait_send()
        g_copy(c).wait_send()
        for k in range(1, ny):
            y_copy(k, c).wait_send()

    @pl.loop(0, nz)
    def _(k):
        for copy in x_copies(k):
            copy.wait_send()

    @pl.loop(0, nz - 1)
    def _(k):
        for copy in z_copies(k):
            copy.wait_send()

    @pl.loop(1, nm)
    def _(k):
        m_copy(k).wait_send()

    @pl.loop(1, nd)
    def _(k):
        p_copy(k).wait_send()


def per_device(
    nd, nm,
    hidden_activation,
    target_head_rows,
    reference_log_probability,
    response_token_mask,
    sequence_tile_lengths,
    pair_destination,
    adapter_down_first,
    adapter_down_second,
):
    micro_count, pairs_dev, _, seq, ff = hidden_activation.shape
    width = target_head_rows.shape[-1]
    rank = adapter_down_first.shape[1]
    tokens = micro_count * pairs_dev * 2 * seq
    chunks = tokens // seq
    ny, nz = nm // CORES, nd // SIDES
    ra, rb = ff // nd, width // nd
    positions = jnp.arange(seq) // TILE
    live = ((response_token_mask == 1) & (positions < sequence_tile_lengths[..., None])).astype(F32)
    vmem = pl.BlockSpec(memory_space=pltpu.VMEM)
    hbm = pl.BlockSpec(memory_space=pl.ANY)
    V = pltpu.VMEM
    dma = pltpu.SemaphoreType.DMA
    bf16 = jnp.bfloat16
    raw_a, raw_b, stats = pl.pallas_call(
        functools.partial(kernel, nd, nm, seq),
        out_shape=(
            jax.ShapeDtypeStruct((ra, rank), F32),
            jax.ShapeDtypeStruct((rb, rank), F32),
            jax.ShapeDtypeStruct((nd, 1, 128), F32),
        ),
        in_specs=[hbm, hbm, vmem, vmem, hbm, hbm],
        out_specs=(vmem, vmem, vmem),
        scratch_shapes=[
            V((tokens, ff), bf16), V((tokens, width), bf16), V((ff, rank), bf16), V((width, rank), bf16),
            V((2, tokens, rank), F32), V((tokens, rank), F32), V((tokens, rank), F32),
            V((ny - 1, tokens, rank), F32), V((2, tokens, rank), F32),
            V((tokens, rank), bf16), V((tokens, rank), bf16), V((ff, rank), F32), V((width, rank), F32),
            V((nz, ra, rank), F32), V((nz, rb, rank), F32), V((nz - 1, ra, rank), F32), V((nz - 1, rb, rank), F32),
            V((1, 128), F32), V((1, 1, 128), F32), V((1, 1, 128), F32), V((nm, 1, 128), F32), V((nd, 1, 128), F32),
            dma((2,)), dma((chunks,)), dma((chunks,)), dma((chunks,)), dma((chunks,)),
            dma((ny - 1, chunks)), dma((ny - 1, chunks)), dma((chunks,)), dma((chunks,)),
            dma((nz, 2)), dma((nz, 2)), dma((nz - 1, 2)), dma((nz - 1, 2)),
            dma((nm - 1,)), dma((nm - 1,)), dma((nd - 1,)), dma((nd - 1,)),
        ],
        compiler_params=pltpu.CompilerParams(collective_id=0, has_side_effects=True, vmem_limit_bytes=60 * 2**20),
    )(
        hidden_activation.reshape(tokens, ff),
        target_head_rows.reshape(tokens, width),
        reference_log_probability.reshape(tokens, 1),
        live.reshape(tokens, 1),
        adapter_down_first,
        adapter_down_second,
    )
    stats = stats[:, 0, :]
    pairs = micro_count * pairs_dev
    all_margins = (
        stats[:, 1 : 1 + pairs].reshape(nd, micro_count, pairs_dev).transpose(1, 0, 2).reshape(micro_count, -1)
    )
    targets = lax.axis_index("dp") * pairs_dev + jnp.arange(pairs_dev)
    hits = pair_destination[:, :, None] == targets[None, None, :]
    pair_margin = jnp.sum(jnp.where(hits, all_margins[:, :, None], 0.0), axis=1)
    mean_loss = jnp.mean(jax.nn.softplus(-all_margins))
    scale = 1.0 / jnp.sqrt(jnp.sum(stats[:, 0]) / ((ff + width) * nm * rank) + 1e-06)
    return (pair_margin, mean_loss, raw_a * scale, raw_b * scale)


def solution(mesh):
    in_specs = (
        P(None, "dp", None, None, "mp"),
        P(None, "dp", None, None, "mp"),
        P(None, "dp", None, None),
        P(None, "dp", None, None),
        P(None, "dp", None),
        P(),
        P("mp", None),
        P("mp", None),
    )
    out_specs = (P(None, "dp"), P(), P(("mp", "dp"), None), P(("mp", "dp"), None))
    return jax.shard_map(
        functools.partial(per_device, mesh.shape["dp"], mesh.shape["mp"]),
        mesh=mesh, in_specs=in_specs, out_specs=out_specs, check_vma=False,
    )
```

```python
import functools
import math

import jax
import jax.numpy as jnp
from jax import lax
from jax.experimental import pallas as pl
from jax.experimental.pallas import tpu as pltpu
from jax.sharding import PartitionSpec as P

TILE = 128
BETA = 0.1
CORES = 2
SIDES = 2
F32 = jnp.float32
MESH = pl.DeviceIdType.MESH
TRANSPOSED = (((0,), (0,)), ((), ()))


def remote(src, dst, send, recv, target):
    return pltpu.make_async_remote_copy(
        src_ref=src, dst_ref=dst, send_sem=send, recv_sem=recv, device_id=target, device_id_type=MESH
    )


def block_of(size):
    return next(width for width in (512, 256, 128, size) if size % width == 0)


def kernel(
    nd, nm, seq,
    hid_ref, rows_ref, token_ref, wa_ref, wb_ref,
    out_a, out_b, out_stats,
    hid, rows, wa, wb, parts, d2d_in, pair_sum, y_in, full, d_lat, d_read, raw_a, raw_b,
    xin_a, xin_b, lin_a, lin_b, rin_a, rin_b, ref_col, live_col, margin_row, mine, mine_dp, stats_mp, stats_dp,
    load_w, load_h, load_r, d2d_s, d2d_r, y_s, y_r, g_s, g_r, x_s, x_r, z_s, l_r, r_r, m_s, m_r, p_s, p_r,
):
    tokens, rank = hid.shape[0], wa.shape[1]
    chunks = tokens // seq
    ny, nz = nm // CORES, nd // SIDES
    dp, mp = lax.axis_index("dp"), lax.axis_index("mp")
    core, y = mp % CORES, mp // CORES
    side, z = dp % SIDES, dp // SIDES
    ra, rb = out_a.shape[0], out_b.shape[0]
    root = math.sqrt(rank)

    def span(c):
        return pl.ds(c * seq, seq)

    loads = [
        pltpu.make_async_copy(wa_ref, wa, load_w.at[0]),
        pltpu.make_async_copy(wb_ref, wb, load_w.at[1]),
    ]
    load_hid = [pltpu.make_async_copy(hid_ref.at[span(c)], hid.at[span(c)], load_h.at[c]) for c in range(chunks)]
    load_rows = [pltpu.make_async_copy(rows_ref.at[span(c)], rows.at[span(c)], load_r.at[c]) for c in range(chunks)]
    loads[0].start()
    load_hid[0].start()
    loads[1].start()
    load_rows[0].start()
    for c in range(1, chunks):
        load_hid[c].start()
        load_rows[c].start()

    columns = jnp.transpose(token_ref[...])
    place = lax.broadcasted_iota(jnp.int32, columns.shape, 1)
    for c in range(chunks):
        ref_col[span(c), :] = jnp.sum(jnp.where(place == c, columns, 0.0), axis=1, keepdims=True)
        live_col[span(c), :] = jnp.sum(jnp.where(place == chunks + c, columns, 0.0), axis=1, keepdims=True)

    barrier = pltpu.get_barrier_semaphore()

    @pl.loop(1, nm)
    def _(k):
        pl.semaphore_signal(barrier, inc=1, device_id=(dp, (mp + k) % nm), device_id_type=MESH)

    @pl.loop(1, nd)
    def _(k):
        pl.semaphore_signal(barrier, inc=1, device_id=((dp + k) % nd, mp), device_id_type=MESH)

    pl.semaphore_wait(barrier, nm + nd - 2)

    partner = (dp, y * CORES + (1 - core))

    def d2d_copy(c):
        return remote(parts.at[1 - core, span(c)], d2d_in.at[span(c)], d2d_s.at[c], d2d_r.at[c], partner)

    def y_copy(k, c):
        target = (dp, ((y + k) % ny) * CORES + core)
        return remote(pair_sum.at[span(c)], y_in.at[ny - 1 - k, span(c)], y_s.at[k - 1, c], y_r.at[ny - 1 - k, c], target)

    def g_copy(c):
        return remote(full.at[core, span(c)], full.at[core, span(c)], g_s.at[c], g_r.at[c], partner)

    def g_arrival(c):
        here = full.at[1 - core, span(c)]
        return remote(here, here, g_s.at[c], g_r.at[c], partner)

    def forward(c):
        d2d_copy(c).wait_recv()
        pair_sum[span(c), :] = parts[core, span(c), :] + d2d_in[span(c), :]
        for k in range(1, ny):
            y_copy(k, c).start()

    for c in range(chunks):
        if c == 0:
            loads[0].wait()
        load_hid[c].wait()
        parts[0, span(c), :] = jnp.dot(hid[span(c), :], wa[...], preferred_element_type=F32)
        if c == 0:
            loads[1].wait()
        load_rows[c].wait()
        parts[1, span(c), :] = jnp.dot(rows[span(c), :], wb[...], preferred_element_type=F32)
        d2d_copy(c).start()
        if c:
            forward(c - 1)
    forward(chunks - 1)

    margin_row[...] = jnp.zeros_like(margin_row)
    lane = lax.broadcasted_iota(jnp.int32, margin_row.shape, 1)
    sign = jnp.where(lax.broadcasted_iota(jnp.int32, (2 * seq, 1), 0) < seq, 1.0, -1.0).astype(F32)

    def gradient(both, source, slopes, total, first):
        width = block_of(total.shape[0])

        @pl.loop(0, total.shape[0] // width)
        def _(j):
            at = pl.ds(pl.multiple_of(j * width, width), width)
            term = lax.dot_general(source[both, at], slopes[both, :], TRANSPOSED, preferred_element_type=F32)
            total[at, :] = term if first else total[at, :] + term

    def at(d, which):
        size = rb if which else ra
        return pl.ds(pl.multiple_of(d * size, 8), size)

    def order(k):
        high = (2 * z) // nz
        low_z = z + high * (nz - 1 - 2 * z)
        d = nz - 1 - k - (k + low_z) // max(nz - 1, 1)
        return d + high * (nz - 1 - 2 * d)

    def x_copy(k, d, which):
        raw, xin = (raw_b, xin_b) if which else (raw_a, xin_a)
        source = raw.at[at(d * SIDES + (1 - side), which)]
        return remote(source, xin.at[k], x_s.at[k, which], x_r.at[k, which], (z * SIDES + (1 - side), mp))

    def l_copy(k, d, which):
        xin, lin = (xin_b, lin_b) if which else (xin_a, lin_a)
        target = (((z + 1) % nz) * SIDES + side, mp)
        return remote(xin.at[k], lin.at[d], z_s.at[k, which], l_r.at[d, which], target)

    def r_copy(k, d, which):
        xin, rin = (xin_b, rin_b) if which else (xin_a, rin_a)
        target = (((z + nz - 1) % nz) * SIDES + side, mp)
        return remote(xin.at[k], rin.at[d], z_s.at[k, which], r_r.at[d, which], target)

    def start_x(which):
        @pl.loop(0, nz - 1)
        def _(k):
            x_copy(k, order(k), which).start()

        x_copy(nz - 1, z, which).start()

    for p in range(chunks // 2):
        for c in (2 * p, 2 * p + 1):
            value = pair_sum[span(c), :]
            for k in range(ny - 1, 0, -1):
                y_copy(k, c).wait_recv()
                value = value + y_in[ny - 1 - k, span(c), :]
            full[core, span(c), :] = value
            g_copy(c).start()
        for c in (2 * p, 2 * p + 1):
            g_arrival(c).wait_recv()
        both = pl.ds(2 * p * seq, 2 * seq)
        latent, readout = full[0, both, :], full[1, both, :]
        shift = jnp.sum(latent * readout, axis=1, keepdims=True) / root
        chance = jnp.exp(ref_col[both, :])
        denom = 1.0 - chance + chance * jnp.exp(shift)
        gain = shift - jnp.log(denom)
        live = live_col[both, :]
        margin = BETA * jnp.sum(live * gain * sign, axis=0, keepdims=True)
        slope = -jax.nn.sigmoid(-margin)
        factor = live * (slope * BETA) * sign * (1.0 - chance) / denom / root
        d_lat[both, :] = (factor * readout).astype(jnp.bfloat16)
        d_read[both, :] = (factor * latent).astype(jnp.bfloat16)
        margin_row[...] = jnp.where(lane == p + 1, margin, margin_row[...])
        gradient(both, rows, d_read, raw_b, p == 0)
        if p == chunks // 2 - 1:
            start_x(1)
        gradient(both, hid, d_lat, raw_a, p == 0)
    start_x(0)

    for which in (1, 0):
        raw, xin, lin, rin = (raw_a, xin_a, lin_a, rin_a) if which == 0 else (raw_b, xin_b, lin_b, rin_b)

        @pl.loop(0, nz - 1)
        def _(k):
            d = order(k)
            x_copy(k, d, which).wait_recv()
            xin[k, :, :] = xin[k, :, :] + raw[at(d * SIDES + side, which), :]

            @pl.when(d > z)
            def _():
                @pl.when(z > 0)
                def _():
                    l_copy(k, d, which).wait_recv()
                    xin[k, :, :] = xin[k, :, :] + lin[d, :, :]

                l_copy(k, d, which).start()

            @pl.when(d < z)
            def _():
                @pl.when(z < nz - 1)
                def _():
                    r_copy(k, d, which).wait_recv()
                    xin[k, :, :] = xin[k, :, :] + rin[d, :, :]

                r_copy(k, d, which).start()

    for which in (1, 0):
        raw, xin, lin, rin, out = (
            (raw_a, xin_a, lin_a, rin_a, out_a) if which == 0 else (raw_b, xin_b, lin_b, rin_b, out_b)
        )
        x_copy(nz - 1, z, which).wait_recv()
        out[...] = xin[nz - 1, :, :] + raw[at(dp, which), :]

        @pl.when(z > 0)
        def _():
            l_copy(0, z, which).wait_recv()
            out[...] += lin[z, :, :]

        @pl.when(z < nz - 1)
        def _():
            r_copy(0, z, which).wait_recv()
            out[...] += rin[z, :, :]

    def total_of(value):
        return jnp.sum(jnp.sum(value * value, axis=0, keepdims=True), axis=1, keepdims=True)

    mine[0, :, :] = jnp.where(lane == 0, total_of(out_a[...]) + total_of(out_b[...]), margin_row[...])

    def m_copy(k):
        return remote(mine.at[0], stats_mp.at[mp], m_s.at[k - 1], m_r.at[k - 1], (dp, (mp + k) % nm))

    def p_copy(k):
        return remote(mine_dp.at[0], stats_dp.at[dp], p_s.at[k - 1], p_r.at[k - 1], ((dp + k) % nd, mp))

    @pl.loop(1, nm)
    def _(k):
        m_copy(k).start()

    stats_mp[mp, :, :] = mine[0, :, :]

    @pl.loop(1, nm)
    def _(k):
        m_copy(k).wait_recv()

    squares = stats_mp[0, :, :]
    for k in range(1, nm):
        squares = squares + stats_mp[k, :, :]
    mine_dp[0, :, :] = jnp.where(lane == 0, squares, stats_mp[0, :, :])

    @pl.loop(1, nd)
    def _(k):
        p_copy(k).start()

    stats_dp[dp, :, :] = mine_dp[0, :, :]

    @pl.loop(1, nd)
    def _(k):
        p_copy(k).wait_recv()

    out_stats[...] = stats_dp[...]
    squared = stats_dp[0, :, :]
    for k in range(1, nd):
        squared = squared + stats_dp[k, :, :]
    squared = jnp.sum(jnp.where(lane == 0, squared, 0.0), axis=1, keepdims=True)
    count = (raw_a.shape[0] + raw_b.shape[0]) * nm * rank
    scale = 1.0 / jnp.sqrt(squared / count + 1e-06)
    out_a[...] = out_a[...] * scale
    out_b[...] = out_b[...] * scale

    for c in range(chunks):
        d2d_copy(c).wait_send()
        g_copy(c).wait_send()
        for k in range(1, ny):
            y_copy(k, c).wait_send()

    for which in (1, 0):

        @pl.loop(0, nz)
        def _(k):
            x_copy(k, z, which).wait_send()

        @pl.loop(0, nz - 1)
        def _(k):
            l_copy(k, z, which).wait_send()

    @pl.loop(1, nm)
    def _(k):
        m_copy(k).wait_send()

    @pl.loop(1, nd)
    def _(k):
        p_copy(k).wait_send()


def per_device(
    nd, nm,
    hidden_activation,
    target_head_rows,
    reference_log_probability,
    response_token_mask,
    sequence_tile_lengths,
    pair_destination,
    adapter_down_first,
    adapter_down_second,
):
    micro_count, pairs_dev, _, seq, ff = hidden_activation.shape
    width = target_head_rows.shape[-1]
    rank = adapter_down_first.shape[1]
    tokens = micro_count * pairs_dev * 2 * seq
    chunks = tokens // seq
    ny, nz = nm // CORES, nd // SIDES
    ra, rb = ff // nd, width // nd
    positions = jnp.arange(seq) // TILE
    live = ((response_token_mask == 1) & (positions < sequence_tile_lengths[..., None])).astype(F32)
    vmem = pl.BlockSpec(memory_space=pltpu.VMEM)
    hbm = pl.BlockSpec(memory_space=pl.ANY)
    V = pltpu.VMEM
    dma = pltpu.SemaphoreType.DMA
    bf16 = jnp.bfloat16
    grad_a, grad_b, stats = pl.pallas_call(
        functools.partial(kernel, nd, nm, seq),
        out_shape=(
            jax.ShapeDtypeStruct((ra, rank), F32),
            jax.ShapeDtypeStruct((rb, rank), F32),
            jax.ShapeDtypeStruct((nd, 1, 128), F32),
        ),
        in_specs=[hbm, hbm, vmem, hbm, hbm],
        out_specs=(vmem, vmem, vmem),
        scratch_shapes=[
            V((tokens, ff), bf16), V((tokens, width), bf16), V((ff, rank), bf16), V((width, rank), bf16),
            V((2, tokens, rank), F32), V((tokens, rank), F32), V((tokens, rank), F32),
            V((ny - 1, tokens, rank), F32), V((2, tokens, rank), F32),
            V((tokens, rank), bf16), V((tokens, rank), bf16), V((ff, rank), F32), V((width, rank), F32),
            V((nz, ra, rank), F32), V((nz, rb, rank), F32), V((nz, ra, rank), F32), V((nz, rb, rank), F32),
            V((nz, ra, rank), F32), V((nz, rb, rank), F32), V((tokens, 1), F32), V((tokens, 1), F32),
            V((1, 128), F32), V((1, 1, 128), F32), V((1, 1, 128), F32), V((nm, 1, 128), F32), V((nd, 1, 128), F32),
            dma((2,)), dma((chunks,)), dma((chunks,)), dma((chunks,)), dma((chunks,)),
            dma((ny - 1, chunks)), dma((ny - 1, chunks)), dma((chunks,)), dma((chunks,)),
            dma((nz, 2)), dma((nz, 2)), dma((nz - 1, 2)), dma((nz, 2)), dma((nz, 2)),
            dma((nm - 1,)), dma((nm - 1,)), dma((nd - 1,)), dma((nd - 1,)),
        ],
        compiler_params=pltpu.CompilerParams(collective_id=0, has_side_effects=True, vmem_limit_bytes=60 * 2**20),
    )(
        hidden_activation.reshape(tokens, ff),
        target_head_rows.reshape(tokens, width),
        jnp.concatenate([reference_log_probability.reshape(chunks, seq), live.reshape(chunks, seq)]),
        adapter_down_first,
        adapter_down_second,
    )
    stats = stats[:, 0, :]
    pairs = micro_count * pairs_dev
    all_margins = (
        stats[:, 1 : 1 + pairs].reshape(nd, micro_count, pairs_dev).transpose(1, 0, 2).reshape(micro_count, -1)
    )
    targets = lax.axis_index("dp") * pairs_dev + jnp.arange(pairs_dev)
    hits = pair_destination[:, :, None] == targets[None, None, :]
    pair_margin = jnp.sum(jnp.where(hits, all_margins[:, :, None], 0.0), axis=1)
    mean_loss = jnp.mean(jax.nn.softplus(-all_margins))
    return (pair_margin, mean_loss, grad_a, grad_b)


def solution(mesh):
    in_specs = (
        P(None, "dp", None, None, "mp"),
        P(None, "dp", None, None, "mp"),
        P(None, "dp", None, None),
        P(None, "dp", None, None),
        P(None, "dp", None),
        P(),
        P("mp", None),
        P("mp", None),
    )
    out_specs = (P(None, "dp"), P(), P(("mp", "dp"), None), P(("mp", "dp"), None))
    return jax.shard_map(
        functools.partial(per_device, mesh.shape["dp"], mesh.shape["mp"]),
        mesh=mesh, in_specs=in_specs, out_specs=out_specs, check_vma=False,
    )
```
